256 devices in a mesh: blk: 128 (over y, x_lo, z, core), shard: 2 (over x_hi).
Axes of the slice: x: 4 (x_hi: 2, x_lo: 2; x = x_hi * 2 + x_lo), y: 4, z: 8, core: 2. Of those that a mesh axis runs over, the one named last changes fastest.
Arguments:
- cut_acts: bfloat16 [65536, 1024], P('blk'), may hold values from -6 to 6
- upstream: bfloat16 [65536, 1024], P('blk', 'shard'), may hold values from -1 to 1
- weights: bfloat16 [128, 1024, 1024], P('blk', None, 'shard'), may hold values from -0.59765625 to 0.59765625
- moment_one: float32 [128, 1024, 1024], P('blk', None, 'shard'), may hold values from -6 to 6
- moment_two: float32 [128, 1024, 1024], P('blk', None, 'shard'), may hold values from 1 to 8
Outputs:
- new_weights: bfloat16 [128, 1024, 1024], P('blk', None, 'shard')
- new_moment_one: float32 [128, 1024, 1024], P('blk', None, 'shard')
- new_moment_two: float32 [128, 1024, 1024], P('blk', None, 'shard')
- cut_grads: bfloat16 [3, 65536, 1024], P(None, ('blk', 'shard'))
The draws below stay inside these ranges and needn't reach their ends.
All inputs are finite; a program needn't handle non-finite values.
Results may differ from the reference program's by a relative error of at most 0.0074.
Values may be sent and summed in bfloat16 or wider, within the bound.
A program may use at most 64 MiB of HBM per device.

```python
import math
import jax
import jax.numpy as jnp
from jax import lax

D = 1024
HOPS = 3
ROWS = 512
CLIENTS = 128
TOK_ALL = 65536
N_BLK = 128


def shard_levels(stream_key, dims, split, smallest, top_value):
    factor_of = 1.0
    for dim, shards_of in split:
        draws = jax.random.uniform(jax.random.fold_in(jax.random.fold_in(stream_key, 6), dim), (shards_of,), jnp.float32, smallest / len(split), top_value / len(split))
        factor_of = factor_of * jnp.repeat(jnp.exp(draws), dims[dim] // shards_of).reshape((-1,) + (1,) * (len(dims) - 1 - dim))
    return factor_of


def centred(own_key, dims, spread, most, split=(), dtype=jnp.bfloat16):
    level = shard_levels(own_key, dims, split, -0.22, 0.18) if split else 1.0
    entries = jax.random.normal(own_key, dims, jnp.float32) * spread * level
    return jnp.minimum(jnp.maximum(entries, -most), most).astype(dtype)


def setup_inputs(seed: int = 0) -> dict:
    streams_of = jax.random.split(jax.random.key(seed), 6)
    cut_acts = centred(streams_of[0], (TOK_ALL, D), 1.0, 6.0, ((0, 128),))
    upstream = centred(streams_of[1], (TOK_ALL, D), 0.125, 1.0, ((0, 128), (1, 2)))
    weights = centred(streams_of[2], (CLIENTS, D, D), 0.1, 0.59765625, ((0, 128), (2, 2)))
    moment_one = centred(streams_of[3], (CLIENTS, D, D), 1.0, 6.0, ((0, 128), (2, 2)), jnp.float32)
    moment_two = jnp.clip(jnp.exp(math.log(8.0) - 2.0794415 * jax.random.uniform(streams_of[4], (CLIENTS, D, D), jnp.float32) ** shard_levels(streams_of[4], (CLIENTS, D, D), ((0, 128), (2, 2)), -0.2, 0.2)), 1.0, 8.0)
    return {"cut_acts": cut_acts, "upstream": upstream, "weights": weights, "moment_one": moment_one, "moment_two": moment_two}


def gelu_slope(values):
    inner = 0.7978845608 * (values + 0.044715 * values * values * values)
    tanh_part = jnp.tanh(inner)
    return 0.5 * (1.0 + tanh_part) + 0.5 * values * (1.0 - tanh_part * tanh_part) * 0.7978845608 * (1.0 + 0.134145 * values * values)

def train_hop(operands):
    kernel, first, second, inputs, grad_out = operands
    preact = jnp.dot(inputs, kernel, preferred_element_type=jnp.float32)
    slopes = (grad_out.astype(jnp.float32) * gelu_slope(preact)).astype(jnp.bfloat16)
    gradient = jnp.dot(inputs.T, slopes, preferred_element_type=jnp.float32)
    returned = jnp.dot(slopes, kernel.T, preferred_element_type=jnp.float32).astype(jnp.bfloat16)
    first = 0.9 * first + 0.1 * gradient
    second = 0.95 * second + 0.05 * gradient * gradient
    kernel = (kernel.astype(jnp.float32) - 0.01 * first / (jnp.sqrt(second) + 1e-08)).astype(jnp.bfloat16)
    return (kernel, first, second, returned)

def reference(cut_acts, upstream, weights, moment_one, moment_two):
    acts_split = cut_acts.reshape(N_BLK, ROWS, D)
    grads_split = upstream.reshape(N_BLK, ROWS, D)
    kernel, first, second = (weights, moment_one, moment_two)
    returned_all = []
    for hop_index in range(HOPS):
        shifted_acts = jnp.roll(acts_split, -hop_index, axis=0)
        shifted_grads = jnp.roll(grads_split, -hop_index, axis=0)
        kernel, first, second, returned = lax.map(train_hop, (kernel, first, second, shifted_acts, shifted_grads))
        returned_all.append(jnp.roll(returned, hop_index, axis=0).reshape(TOK_ALL, D))
    return (jnp.roll(kernel, HOPS, axis=0), jnp.roll(first, HOPS, axis=0), jnp.roll(second, HOPS, axis=0), jnp.stack(returned_all))
```

```python
import functools

import jax
import jax.numpy as jnp
from jax import lax
from jax.experimental import pallas as pl
from jax.experimental.pallas import tpu as pltpu
from jax.sharding import PartitionSpec as P

HOPS = 3
D = 1024
N = 512
ROWS = 512
HALF = ROWS // 2
C = 128
Q = N // C
RB = 4
RR = D // RB
RELAYED = 2
Z = 8
MESH = pl.DeviceIdType.MESH
F32 = jnp.float32
BF16 = jnp.bfloat16


def gelu_slope(values):
    square = values * values
    inner = 0.7978845608 * (values + 0.044715 * square * values)
    tanh_part = jnp.tanh(inner)
    return 0.5 * (1.0 + tanh_part) + 0.5 * values * (1.0 - tanh_part * tanh_part) * 0.7978845608 * (
        1.0 + 0.134145 * square
    )


def kernel(
    acts_hbm,
    up_hbm,
    w_hbm,
    m_hbm,
    v_hbm,
    w_out,
    m_out,
    v_out,
    cut_out,
    x_ref,
    xt_ref,
    g_ref,
    w0_ref,
    m0_ref,
    v0_ref,
    arrived,
    leaving,
    relay,
    s_ref,
    own,
    theirs,
    given,
    x_sem,
    g_sem,
    w_sem,
    m_sem,
    v_sem,
    send_sem,
    recv_sem,
    relay_send_sem,
    relay_recv_sem,
    cut_send_sem,
    cut_recv_sem,
):
    n_blk = lax.axis_size("blk")
    me = lax.axis_index("blk")
    side = lax.axis_index("shard")
    after = lax.rem(me + 1, n_blk)
    before = lax.rem(me + n_blk - 1, n_blk)
    on_chip = lax.rem(me, 2)
    depth = lax.rem(me // 2, Z)
    turns = jnp.logical_and(on_chip == 1, depth == Z - 1)
    relays = jnp.logical_and(on_chip == 0, depth == Z - 1)
    lands = jnp.logical_and(on_chip == 0, depth == 0)
    via = lax.rem(me + 2 * Z - 1, n_blk)
    source = lax.rem(me + n_blk - 2 * Z + 1, n_blk)
    landing = lax.rem(me + n_blk - 2 * (Z - 1), n_blk)
    relayer = lax.rem(me + 2 * (Z - 1), n_blk)

    barrier = pltpu.get_barrier_semaphore()

    def greet(index):
        pl.semaphore_signal(barrier, inc=1, device_id={"blk": index}, device_id_type=MESH)

    greet(after)
    greet(before)
    pl.semaphore_signal(barrier, inc=1, device_id={"shard": 1 - side}, device_id_type=MESH)

    @pl.when(turns)
    def _():
        greet(via)

    @pl.when(relays)
    def _():
        greet(source)
        greet(landing)

    @pl.when(lands)
    def _():
        greet(relayer)

    def columns(q):
        return pl.ds(pl.multiple_of(q * C, C), C)

    def load_x():
        return pltpu.make_async_copy(acts_hbm, x_ref, x_sem)

    def load_w(q):
        return pltpu.make_async_copy(w_hbm.at[0, :, columns(q)], w0_ref.at[q], w_sem.at[q])

    def load_g(q):
        return pltpu.make_async_copy(up_hbm.at[:, columns(q)], g_ref.at[q], g_sem.at[q])

    def load_m(q):
        return pltpu.make_async_copy(m_hbm.at[0, :, columns(q)], m0_ref.at[q], m_sem.at[q])

    def load_v(q):
        return pltpu.make_async_copy(v_hbm.at[0, :, columns(q)], v0_ref.at[q], v_sem.at[q])

    load_x().start()
    for q in range(Q):
        load_w(q).start()
        load_g(q).start()
        load_m(q).start()
        load_v(q).start()

    def rows(r):
        return slice(r * RR, (r + 1) * RR)

    def onward(h, q, r):
        return pltpu.make_async_remote_copy(
            src_ref=leaving.at[h, q, :, rows(r)],
            dst_ref=arrived.at[h, q, :, rows(r)],
            send_sem=send_sem.at[h, q, r],
            recv_sem=recv_sem.at[h, q, r],
            device_id={"blk": after},
            device_id_type=MESH,
        )

    def to_relay(h, q, r):
        return pltpu.make_async_remote_copy(
            src_ref=leaving.at[h, q, :, rows(r)],
            dst_ref=relay.at[h, q, r - RB + RELAYED],
            send_sem=send_sem.at[h, q, r],
            recv_sem=relay_recv_sem.at[h, q, r - RB + RELAYED],
            device_id={"blk": via},
            device_id_type=MESH,
        )

    def from_relay(h, q, r):
        return pltpu.make_async_remote_copy(
            src_ref=relay.at[h, q, r - RB + RELAYED],
            dst_ref=arrived.at[h, q, :, rows(r)],
            send_sem=relay_send_sem.at[h, q, r - RB + RELAYED],
            recv_sem=recv_sem.at[h, q, r],
            device_id={"blk": landing},
            device_id_type=MESH,
        )

    def send(h, q, r):
        if r < RB - RELAYED:
            onward(h, q, r).start()
        else:

            @pl.when(turns)
            def _():
                to_relay(h, q, r).start()

            @pl.when(jnp.logical_not(turns))
            def _():
                onward(h, q, r).start()

    def pass_on(h, q):
        @pl.when(relays)
        def _():
            for r in range(RB - RELAYED, RB):
                to_relay(h, q, r).wait_recv()
                from_relay(h, q, r).start()

    def slopes(q, weight):
        preact = jnp.dot(x_ref[...], weight, preferred_element_type=F32)
        s_ref[q] = (g_ref[q].astype(F32) * gelu_slope(preact)).astype(BF16)

    def update(h, q, r, weight, first, second):
        grad = jnp.dot(xt_ref[rows(r), :], s_ref[q], preferred_element_type=F32)
        first = 0.9 * first + 0.1 * grad
        second = 0.95 * second + 0.05 * grad * grad
        leaving[h, q, 0, rows(r)] = (weight.astype(F32) - 0.01 * first / (jnp.sqrt(second) + 1e-08)).astype(BF16)
        leaving[h, q, 1, rows(r)] = first.astype(BF16)
        leaving[h, q, 2, rows(r)] = second.astype(BF16)
        send(h, q, r)

    def cut(h):
        return pltpu.make_async_remote_copy(
            src_ref=given.at[h],
            dst_ref=theirs.at[h],
            send_sem=cut_send_sem.at[h],
            recv_sem=cut_recv_sem.at[h],
            device_id={"shard": 1 - side},
            device_id_type=MESH,
        )

    def cut_part(weights, start, block):
        s_part = jnp.concatenate([s_ref[q, pl.ds(start, HALF), :] for q in range(Q)], axis=1)
        w_part = jnp.concatenate([weights(q)[rows(block), :] for q in range(Q)], axis=1)
        return lax.dot_general(s_part, w_part, (((1,), (1,)), ((), ())), preferred_element_type=F32)

    def cut_grads(h, weights):
        mine = pl.multiple_of(side * HALF, HALF)
        others = pl.multiple_of((1 - side) * HALF, HALF)
        for block in range(RB):
            given[h, :, rows(block)] = cut_part(weights, others, block).astype(BF16)
        cut(h).start()
        for block in range(RB):
            own[h, :, rows(block)] = cut_part(weights, mine, block)

    def cut_done(h):
        cut(h).wait_recv()
        cut_out[h] = (own[h] + theirs[h].astype(F32)).astype(BF16)

    load_x().wait()

    def hop_start(q):
        load_w(q).wait()
        load_g(q).wait()
        slopes(q, w0_ref[q])

    def hop_rest(q):
        load_m(q).wait()
        load_v(q).wait()
        for r in range(RB):
            update(0, q, r, w0_ref[q, rows(r)], m0_ref[q, rows(r)], v0_ref[q, rows(r)])

    hop_start(0)
    for r in range(RB):
        xt_ref[rows(r), :] = x_ref[:, rows(r)].T
    pl.semaphore_wait(
        barrier,
        3 + turns.astype(jnp.int32) + 2 * relays.astype(jnp.int32) + lands.astype(jnp.int32),
    )
    hop_rest(0)

    @pl.loop(1, Q)
    def _(q):
        hop_start(q)
        hop_rest(q)

    cut_grads(0, lambda q: w0_ref.at[q])

    for h in range(1, HOPS):

        @pl.loop(0, Q)
        def _(q):
            pass_on(h - 1, q)
            for r in range(RB):
                onward(h - 1, q, r).wait_recv()
            slopes(q, arrived[h - 1, q, 0])
            for r in range(RB):
                update(
                    h,
                    q,
                    r,
                    arrived[h - 1, q, 0, rows(r)],
                    arrived[h - 1, q, 1, rows(r)].astype(F32),
                    arrived[h - 1, q, 2, rows(r)].astype(F32),
                )

        cut_grads(h, lambda q: arrived.at[h - 1, q, 0])
        cut_done(h - 1)

    def settle(q):
        pass_on(HOPS - 1, q)
        for r in range(RB):
            onward(HOPS - 1, q, r).wait_recv()
            w_out[rows(r), columns(q)] = arrived[HOPS - 1, q, 0, rows(r)]
            m_out[rows(r), columns(q)] = arrived[HOPS - 1, q, 1, rows(r)].astype(F32)
            v_out[rows(r), columns(q)] = arrived[HOPS - 1, q, 2, rows(r)].astype(F32)

    @pl.loop(0, 2)
    def _(q):
        settle(q)

    cut_done(HOPS - 1)

    @pl.loop(2, Q)
    def _(q):
        settle(q)

    for h in range(HOPS):
        cut(h).wait_send()

        @pl.loop(0, Q)
        def _(q):
            for r in range(RB):
                onward(h, q, r).wait_send()

            @pl.when(relays)
            def _():
                for r in range(RB - RELAYED, RB):
                    from_relay(h, q, r).wait_send()


def shards(cut_acts, upstream, weights, moment_one, moment_two):
    anywhere = pl.BlockSpec(memory_space=pl.ANY)
    held = pl.BlockSpec(memory_space=pltpu.VMEM)
    kernel_out, first, second, cuts = pl.pallas_call(
        kernel,
        out_shape=(
            pltpu.VMEM((D, N), BF16),
            pltpu.VMEM((D, N), F32),
            pltpu.VMEM((D, N), F32),
            pltpu.VMEM((HOPS, HALF, D), BF16),
        ),
        in_specs=[anywhere] * 5,
        out_specs=(held,) * 4,
        scratch_shapes=[
            pltpu.VMEM((ROWS, D), BF16),
            pltpu.VMEM((D, ROWS), BF16),
            pltpu.VMEM((Q, ROWS, C), BF16),
            pltpu.VMEM((Q, D, C), BF16),
            pltpu.VMEM((Q, D, C), F32),
            pltpu.VMEM((Q, D, C), F32),
            pltpu.VMEM((HOPS, Q, 3, D, C), BF16),
            pltpu.VMEM((HOPS, Q, 3, D, C), BF16),
            pltpu.VMEM((HOPS, Q, RELAYED, 3, RR, C), BF16),
            pltpu.VMEM((Q, ROWS, C), BF16),
            pltpu.VMEM((HOPS, HALF, D), F32),
            pltpu.VMEM((HOPS, HALF, D), BF16),
            pltpu.VMEM((HOPS, HALF, D), BF16),
            pltpu.SemaphoreType.DMA,
            pltpu.SemaphoreType.DMA((Q,)),
            pltpu.SemaphoreType.DMA((Q,)),
            pltpu.SemaphoreType.DMA((Q,)),
            pltpu.SemaphoreType.DMA((Q,)),
            pltpu.SemaphoreType.DMA((HOPS, Q, RB)),
            pltpu.SemaphoreType.DMA((HOPS, Q, RB)),
            pltpu.SemaphoreType.DMA((HOPS, Q, RELAYED)),
            pltpu.SemaphoreType.DMA((HOPS, Q, RELAYED)),
            pltpu.SemaphoreType.DMA((HOPS,)),
            pltpu.SemaphoreType.DMA((HOPS,)),
        ],
        compiler_params=pltpu.CompilerParams(
            collective_id=0, has_side_effects=True, vmem_limit_bytes=48 * 2**20
        ),
        name="relay_train",
    )(cut_acts, upstream, weights, moment_one, moment_two)
    return kernel_out[None], first[None], second[None], cuts


def solution(mesh):
    placed = (
        P("blk", None),
        P("blk", "shard"),
        P("blk", None, "shard"),
        P("blk", None, "shard"),
        P("blk", None, "shard"),
    )
    return jax.shard_map(
        shards,
        mesh=mesh,
        in_specs=placed,
        out_specs=(
            P("blk", None, "shard"),
            P("blk", None, "shard"),
            P("blk", None, "shard"),
            P(None, ("blk", "shard"), None),
        ),
        check_vma=False,
    )
```

```python
import functools

import jax
import jax.numpy as jnp
from jax import lax
from jax.experimental import pallas as pl
from jax.experimental.pallas import tpu as pltpu
from jax.sharding import PartitionSpec as P

HOPS = 3
D = 1024
N = 512
ROWS = 512
HALF = ROWS // 2
C = 128
Q = N // C
RB = 4
RR = D // RB
RELAYED = 3
TURNED = (2, 2)
Z = 8
BACKWARD = (2, 2, 1)
MESH = pl.DeviceIdType.MESH
F32 = jnp.float32
BF16 = jnp.bfloat16


def gelu_slope(values):
    square = values * values
    inner = 0.7978845608 * (values + 0.044715 * square * values)
    tanh_part = jnp.tanh(inner)
    return 0.5 * (1.0 + tanh_part) + 0.5 * values * (1.0 - tanh_part * tanh_part) * 0.7978845608 * (
        1.0 + 0.134145 * square
    )


def kernel(
    acts_hbm,
    up_hbm,
    w_hbm,
    m_hbm,
    v_hbm,
    w_out,
    m_out,
    v_out,
    cut_out,
    x_ref,
    xt_ref,
    g_ref,
    w0_ref,
    m0_ref,
    v0_ref,
    arrived,
    leaving,
    relay,
    back,
    s_ref,
    own,
    theirs,
    given,
    x_sem,
    g_sem,
    w_sem,
    m_sem,
    v_sem,
    send_sem,
    recv_sem,
    relay_send_sem,
    relay_recv_sem,
    back_send_sem,
    back_recv_sem,
    cut_send_sem,
    cut_recv_sem,
):
    n_blk = lax.axis_size("blk")
    me = lax.axis_index("blk")
    side = lax.axis_index("shard")
    after = lax.rem(me + 1, n_blk)
    before = lax.rem(me + n_blk - 1, n_blk)
    on_chip = lax.rem(me, 2)
    depth = lax.rem(me // 2, Z)
    turns = jnp.logical_and(on_chip == 1, depth == Z - 1)
    relays = jnp.logical_and(on_chip == 0, depth == Z - 1)
    lands = jnp.logical_and(on_chip == 0, depth == 0)
    via = lax.rem(me + 2 * Z - 1, n_blk)
    source = lax.rem(me + n_blk - 2 * Z + 1, n_blk)
    landing = lax.rem(me + n_blk - 2 * (Z - 1), n_blk)
    relayer = lax.rem(me + 2 * (Z - 1), n_blk)
    odd = lax.rem(depth, 2) == 1
    sends_on = on_chip == 1
    kind = lax.rem(depth + 1, 2)
    helps = jnp.logical_and(sends_on, odd)

    def chip(here, by):
        return lax.rem(here + n_blk + 2 * by, n_blk)

    helper = jnp.where(
        odd,
        chip(me, jnp.where(depth == 5, -4, 4)),
        chip(me, jnp.where(depth <= 2, 5, -3)),
    )
    back_sources = (
        chip(me, jnp.where(depth == 1, 4, -4)),
        chip(me, jnp.where(depth >= 5, -5, 3)),
    )
    back_landings = (
        chip(me - 1, jnp.where(depth == 1, 5, -3)),
        chip(me - 1, jnp.where(depth >= 5, -4, 4)),
    )
    last_z = lax.rem(depth + Z - 1, Z)
    back_helper = chip(
        me + 1,
        jnp.where(
            lax.rem(last_z, 2) == 1,
            jnp.where(last_z == 5, -5, 3),
            jnp.where(last_z <= 2, 4, -4),
        ),
    )

    barrier = pltpu.get_barrier_semaphore()

    def greet(index):
        pl.semaphore_signal(barrier, inc=1, device_id={"blk": index}, device_id_type=MESH)

    greet(after)
    greet(before)
    pl.semaphore_signal(barrier, inc=1, device_id={"shard": 1 - side}, device_id_type=MESH)

    @pl.when(turns)
    def _():
        greet(via)

    @pl.when(relays)
    def _():
        greet(source)
        greet(landing)

    @pl.when(lands)
    def _():
        greet(relayer)

    @pl.when(sends_on)
    def _():
        greet(helper)

    @pl.when(on_chip == 0)
    def _():
        greet(back_helper)

    @pl.when(helps)
    def _():
        for index in back_sources + back_landings:
            greet(index)

    def columns(q):
        return pl.ds(pl.multiple_of(q * C, C), C)

    def load_x():
        return pltpu.make_async_copy(acts_hbm, x_ref, x_sem)

    def load_w(q):
        return pltpu.make_async_copy(w_hbm.at[0, :, columns(q)], w0_ref.at[q], w_sem.at[q])

    def load_g(q):
        return pltpu.make_async_copy(up_hbm.at[:, columns(q)], g_ref.at[q], g_sem.at[q])

    def load_m(q):
        return pltpu.make_async_copy(m_hbm.at[0, :, columns(q)], m0_ref.at[q], m_sem.at[q])

    def load_v(q):
        return pltpu.make_async_copy(v_hbm.at[0, :, columns(q)], v0_ref.at[q], v_sem.at[q])

    load_x().start()
    for q in range(Q):
        load_w(q).start()
        load_g(q).start()
        load_m(q).start()
        load_v(q).start()

    def rows(r):
        return slice(r * RR, (r + 1) * RR)

    def onward(h, q, r):
        return pltpu.make_async_remote_copy(
            src_ref=leaving.at[h, q, :, rows(r)],
            dst_ref=arrived.at[h, q, :, rows(r)],
            send_sem=send_sem.at[h, q, r],
            recv_sem=recv_sem.at[h, q, r],
            device_id={"blk": after},
            device_id_type=MESH,
        )

    def to_relay(h, q, r):
        return pltpu.make_async_remote_copy(
            src_ref=leaving.at[h, q, :, rows(r)],
            dst_ref=relay.at[h, q, r - RB + RELAYED],
            send_sem=send_sem.at[h, q, r],
            recv_sem=relay_recv_sem.at[h, q, r - RB + RELAYED],
            device_id={"blk": via},
            device_id_type=MESH,
        )

    def from_relay(h, q, r):
        return pltpu.make_async_remote_copy(
            src_ref=relay.at[h, q, r - RB + RELAYED],
            dst_ref=arrived.at[h, q, :, rows(r)],
            send_sem=relay_send_sem.at[h, q, r - RB + RELAYED],
            recv_sem=recv_sem.at[h, q, r],
            device_id={"blk": landing},
            device_id_type=MESH,
        )

    def to_helper(h, k, r):
        return pltpu.make_async_remote_copy(
            src_ref=leaving.at[h, h, :, rows(r)],
            dst_ref=back.at[h, k, RB - 1 - r],
            send_sem=send_sem.at[h, h, r],
            recv_sem=back_recv_sem.at[h, k, RB - 1 - r],
            device_id={"blk": helper},
            device_id_type=MESH,
        )

    def from_helper(h, k, r):
        return pltpu.make_async_remote_copy(
            src_ref=back.at[h, k, RB - 1 - r],
            dst_ref=arrived.at[h, h, :, rows(r)],
            send_sem=back_send_sem.at[h, k, RB - 1 - r],
            recv_sem=recv_sem.at[h, h, r],
            device_id={"blk": back_landings[k]},
            device_id_type=MESH,
        )

    def help_back(h):
        @pl.when(helps)
        def _():
            for k in (1, 0):
                for r in range(RB - BACKWARD[h], RB):
                    to_helper(h, k, r).wait_recv()
                    from_helper(h, k, r).start()

    def turned(h, q, r):
        in_first = RB - BACKWARD[h] - TURNED[0] <= r < RB - BACKWARD[h]
        in_rest = r >= RB - TURNED[1]
        if in_first and in_rest:
            return q >= 0
        return q == h if in_first else q != h if in_rest else q < 0

    def send(h, q, r):
        if r < RB - RELAYED:
            onward(h, q, r).start()
            return
        backward = jnp.logical_and(sends_on, q == h) if r >= RB - BACKWARD[h] else q < 0
        first = jnp.logical_and(turns, turned(h, q, r))

        @pl.when(backward)
        def _():
            to_helper(h, kind, r).start()

        @pl.when(first)
        def _():
            to_relay(h, q, r).start()

        @pl.when(jnp.logical_not(jnp.logical_or(first, backward)))
        def _():
            onward(h, q, r).start()

    def relayed(h, q, act):
        for r in range(RB - RELAYED, RB):

            @pl.when(jnp.logical_and(relays, turned(h, q, r)))
            def _():
                act(r)

    def pass_on(h, q):
        def act(r):
            to_relay(h, q, r).wait_recv()
            from_relay(h, q, r).start()

        relayed(h, q, act)

    def slopes(q, weight):
        preact = jnp.dot(x_ref[...], weight, preferred_element_type=F32)
        s_ref[q] = (g_ref[q].astype(F32) * gelu_slope(preact)).astype(BF16)

    def update(h, q, r, weight, first, second):
        grad = jnp.dot(xt_ref[rows(r), :], s_ref[q], preferred_element_type=F32)
        first = 0.9 * first + 0.1 * grad
        second = 0.95 * second + 0.05 * grad * grad
        leaving[h, q, 0, rows(r)] = (weight.astype(F32) - 0.01 * first / (jnp.sqrt(second) + 1e-08)).astype(BF16)
        leaving[h, q, 1, rows(r)] = first.astype(BF16)
        leaving[h, q, 2, rows(r)] = second.astype(BF16)
        send(h, q, r)

    def cut(h):
        return pltpu.make_async_remote_copy(
            src_ref=given.at[h],
            dst_ref=theirs.at[h],
            send_sem=cut_send_sem.at[h],
            recv_sem=cut_recv_sem.at[h],
            device_id={"shard": 1 - side},
            device_id_type=MESH,
        )

    def cut_part(weights, start, block):
        s_part = jnp.concatenate([s_ref[q, pl.ds(start, HALF), :] for q in range(Q)], axis=1)
        w_part = jnp.concatenate([weights(q)[rows(block), :] for q in range(Q)], axis=1)
        return lax.dot_general(s_part, w_part, (((1,), (1,)), ((), ())), preferred_element_type=F32)

    def cut_grads(h, weights):
        mine = pl.multiple_of(side * HALF, HALF)
        others = pl.multiple_of((1 - side) * HALF, HALF)
        for block in range(RB):
            given[h, :, rows(block)] = cut_part(weights, others, block).astype(BF16)
        cut(h).start()
        for block in range(RB):
            own[h, :, rows(block)] = cut_part(weights, mine, block)

    def cut_done(h):
        cut(h).wait_recv()
        cut_out[h] = (own[h] + theirs[h].astype(F32)).astype(BF16)

    load_x().wait()

    def hop_start(q):
        load_w(q).wait()
        load_g(q).wait()
        slopes(q, w0_ref[q])

    def hop_rest(q):
        load_m(q).wait()
        load_v(q).wait()
        for r in range(RB):
            update(0, q, r, w0_ref[q, rows(r)], m0_ref[q, rows(r)], v0_ref[q, rows(r)])

    hop_start(0)
    for r in range(RB):
        xt_ref[rows(r), :] = x_ref[:, rows(r)].T
    def one(flag):
        return flag.astype(jnp.int32)

    pl.semaphore_wait(barrier, 4 + one(turns) + 2 * one(relays) + one(lands) + 4 * one(helps))
    hop_rest(0)

    @pl.loop(1, Q)
    def _(q):
        hop_start(q)
        hop_rest(q)

    cut_grads(0, lambda q: w0_ref.at[q])

    def turn(h, i):
        return lax.rem(i + h, Q)

    for h in range(1, HOPS):

        @pl.loop(0, 2 if h == 1 else Q)
        def _(i):
            pass_on(h - 1, turn(h - 1, i))

        @pl.loop(0, Q)
        def _(i):
            q = turn(h, i)
            if h == 1:

                @pl.when(i == 1)
                def _():
                    pass_on(h - 1, turn(h - 1, 2))
                    pass_on(h - 1, turn(h - 1, 3))

            else:

                @pl.when(i == Q - 1)
                def _():
                    @pl.loop(0, Q)
                    def _(k):
                        pass_on(h, turn(h, k))

            for r in range(RB):
                onward(h - 1, q, r).wait_recv()
            slopes(q, arrived[h - 1, q, 0])
            for r in range(RB):
                update(
                    h,
                    q,
                    r,
                    arrived[h - 1, q, 0, rows(r)],
                    arrived[h - 1, q, 1, rows(r)].astype(F32),
                    arrived[h - 1, q, 2, rows(r)].astype(F32),
                )

        help_back(h - 1)
        cut_grads(h, lambda q: arrived.at[h - 1, q, 0])
        cut_done(h - 1)

    def settle(q):
        for r in range(RB):
            onward(HOPS - 1, q, r).wait_recv()
            w_out[rows(r), columns(q)] = arrived[HOPS - 1, q, 0, rows(r)]
            m_out[rows(r), columns(q)] = arrived[HOPS - 1, q, 1, rows(r)].astype(F32)
            v_out[rows(r), columns(q)] = arrived[HOPS - 1, q, 2, rows(r)].astype(F32)

    help_back(HOPS - 1)

    @pl.loop(0, 2)
    def _(i):
        settle(turn(HOPS, i))

    cut_done(HOPS - 1)

    @pl.loop(2, Q)
    def _(i):
        settle(turn(HOPS, i))

    for h in range(HOPS):
        cut(h).wait_send()

        @pl.loop(0, Q)
        def _(q):
            for r in range(RB):
                onward(h, q, r).wait_send()

            relayed(h, q, lambda r: from_relay(h, q, r).wait_send())

        @pl.when(helps)
        def _():
            for r in range(RB - BACKWARD[h], RB):
                for k in range(2):
                    from_helper(h, k, r).wait_send()


def deliver(w_in, m_in, v_in, cut_in, w_out, m_out, v_out, cut_out, sem):
    copies = [
        pltpu.make_async_copy(m_in, m_out.at[0], sem.at[0]),
        pltpu.make_async_copy(v_in, v_out.at[0], sem.at[1]),
        pltpu.make_async_copy(cut_in, cut_out, sem.at[2]),
        pltpu.make_async_copy(w_in, w_out.at[0], sem.at[3]),
    ]
    for copy in copies:
        copy.start()
    for copy in copies:
        copy.wait()


def shards(cut_acts, upstream, weights, moment_one, moment_two):
    anywhere = pl.BlockSpec(memory_space=pl.ANY)
    held = pl.BlockSpec(memory_space=pltpu.VMEM)
    trained = pl.pallas_call(
        kernel,
        out_shape=(
            pltpu.VMEM((D, N), BF16),
            pltpu.VMEM((D, N), F32),
            pltpu.VMEM((D, N), F32),
            pltpu.VMEM((HOPS, HALF, D), BF16),
        ),
        in_specs=[anywhere] * 5,
        out_specs=(held,) * 4,
        scratch_shapes=[
            pltpu.VMEM((ROWS, D), BF16),
            pltpu.VMEM((D, ROWS), BF16),
            pltpu.VMEM((Q, ROWS, C), BF16),
            pltpu.VMEM((Q, D, C), BF16),
            pltpu.VMEM((Q, D, C), F32),
            pltpu.VMEM((Q, D, C), F32),
            pltpu.VMEM((HOPS, Q, 3, D, C), BF16),
            pltpu.VMEM((HOPS, Q, 3, D, C), BF16),
            pltpu.VMEM((HOPS, Q, RELAYED, 3, RR, C), BF16),
            pltpu.VMEM((HOPS, 2, 2, 3, RR, C), BF16),
            pltpu.VMEM((Q, ROWS, C), BF16),
            pltpu.VMEM((HOPS, HALF, D), F32),
            pltpu.VMEM((HOPS, HALF, D), BF16),
            pltpu.VMEM((HOPS, HALF, D), BF16),
            pltpu.SemaphoreType.DMA,
            pltpu.SemaphoreType.DMA((Q,)),
            pltpu.SemaphoreType.DMA((Q,)),
            pltpu.SemaphoreType.DMA((Q,)),
            pltpu.SemaphoreType.DMA((Q,)),
            pltpu.SemaphoreType.DMA((HOPS, Q, RB)),
            pltpu.SemaphoreType.DMA((HOPS, Q, RB)),
            pltpu.SemaphoreType.DMA((HOPS, Q, RELAYED)),
            pltpu.SemaphoreType.DMA((HOPS, Q, RELAYED)),
            pltpu.SemaphoreType.DMA((HOPS, 2, 2)),
            pltpu.SemaphoreType.DMA((HOPS, 2, 2)),
            pltpu.SemaphoreType.DMA((HOPS,)),
            pltpu.SemaphoreType.DMA((HOPS,)),
        ],
        compiler_params=pltpu.CompilerParams(
            collective_id=0, has_side_effects=True, vmem_limit_bytes=48 * 2**20
        ),
        name="relay_train",
    )(cut_acts, upstream, weights, moment_one, moment_two)
    return pl.pallas_call(
        deliver,
        out_shape=(
            jax.ShapeDtypeStruct((1, D, N), BF16),
            jax.ShapeDtypeStruct((1, D, N), F32),
            jax.ShapeDtypeStruct((1, D, N), F32),
            jax.ShapeDtypeStruct((HOPS, HALF, D), BF16),
        ),
        in_specs=[held] * 4,
        out_specs=(anywhere,) * 4,
        scratch_shapes=[pltpu.SemaphoreType.DMA((4,))],
        compiler_params=pltpu.CompilerParams(vmem_limit_bytes=2**20),
        name="deliver",
    )(*trained)


def solution(mesh):
    placed = (
        P("blk", None),
        P("blk", "shard"),
        P("blk", None, "shard"),
        P("blk", None, "shard"),
        P("blk", None, "shard"),
    )
    return jax.shard_map(
        shards,
        mesh=mesh,
        in_specs=placed,
        out_specs=(
            P("blk", None, "shard"),
            P("blk", None, "shard"),
            P("blk", None, "shard"),
            P(None, ("blk", "shard"), None),
        ),
        check_vma=False,
    )
```

```python
import functools

import jax
import jax.numpy as jnp
from jax import lax
from jax.experimental import pallas as pl
from jax.experimental.pallas import tpu as pltpu
from jax.sharding import PartitionSpec as P

HOPS = 3
D = 1024
N = 512
ROWS = 512
HALF = ROWS // 2
C = 128
Q = N // C
RB = 4
RR = D // RB
RELAYED = 3
TURNED = (2, 2)
Z = 8
BACKWARD = (2, 2, 0)
BACKWARD_TURN = (2, 2, 3)
MOST_BACK = max(BACKWARD_TURN)
MESH = pl.DeviceIdType.MESH
F32 = jnp.float32
BF16 = jnp.bfloat16


def gelu_slope(values):
    square = values * values
    inner = 0.7978845608 * (values + 0.044715 * square * values)
    tanh_part = jnp.tanh(inner)
    return 0.5 * (1.0 + tanh_part) + 0.5 * values * (1.0 - tanh_part * tanh_part) * 0.7978845608 * (
        1.0 + 0.134145 * square
    )


def kernel(
    acts_hbm,
    up_hbm,
    w_hbm,
    m_hbm,
    v_hbm,
    w_out,
    m_out,
    v_out,
    cut_out,
    x_ref,
    xt_ref,
    g_ref,
    w0_ref,
    m0_ref,
    v0_ref,
    arrived,
    leaving,
    relay,
    back,
    s_ref,
    own,
    theirs,
    given,
    x_sem,
    g_sem,
    w_sem,
    m_sem,
    v_sem,
    send_sem,
    recv_sem,
    relay_send_sem,
    relay_recv_sem,
    back_send_sem,
    back_recv_sem,
    cut_send_sem,
    cut_recv_sem,
):
    n_blk = lax.axis_size("blk")
    me = lax.axis_index("blk")
    side = lax.axis_index("shard")
    after = lax.rem(me + 1, n_blk)
    before = lax.rem(me + n_blk - 1, n_blk)
    on_chip = lax.rem(me, 2)
    depth = lax.rem(me // 2, Z)
    turns = jnp.logical_and(on_chip == 1, depth == Z - 1)
    relays = jnp.logical_and(on_chip == 0, depth == Z - 1)
    lands = jnp.logical_and(on_chip == 0, depth == 0)
    via = lax.rem(me + 2 * Z - 1, n_blk)
    source = lax.rem(me + n_blk - 2 * Z + 1, n_blk)
    landing = lax.rem(me + n_blk - 2 * (Z - 1), n_blk)
    relayer = lax.rem(me + 2 * (Z - 1), n_blk)
    odd = lax.rem(depth, 2) == 1
    sends_on = on_chip == 1
    kind = lax.rem(depth + 1, 2)
    helps = jnp.logical_and(sends_on, odd)

    def chip(here, by):
        return lax.rem(here + n_blk + 2 * by, n_blk)

    helper = jnp.where(
        odd,
        chip(me, jnp.where(depth == 5, -4, 4)),
        chip(me, jnp.where(depth <= 2, 5, -3)),
    )
    back_sources = (
        chip(me, jnp.where(depth == 1, 4, -4)),
        chip(me, jnp.where(depth >= 5, -5, 3)),
    )
    back_landings = (
        chip(me - 1, jnp.where(depth == 1, 5, -3)),
        chip(me - 1, jnp.where(depth >= 5, -4, 4)),
    )
    last_z = lax.rem(depth + Z - 1, Z)
    back_helper = chip(
        me + 1,
        jnp.where(
            lax.rem(last_z, 2) == 1,
            jnp.where(last_z == 5, -5, 3),
            jnp.where(last_z <= 2, 4, -4),
        ),
    )

    barrier = pltpu.get_barrier_semaphore()

    def greet(index):
        pl.semaphore_signal(barrier, inc=1, device_id={"blk": index}, device_id_type=MESH)

    greet(after)
    greet(before)
    pl.semaphore_signal(barrier, inc=1, device_id={"shard": 1 - side}, device_id_type=MESH)

    @pl.when(turns)
    def _():
        greet(via)

    @pl.when(relays)
    def _():
        greet(source)
        greet(landing)

    @pl.when(lands)
    def _():
        greet(relayer)

    @pl.when(sends_on)
    def _():
        greet(helper)

    @pl.when(on_chip == 0)
    def _():
        greet(back_helper)

    @pl.when(helps)
    def _():
        for index in back_sources + back_landings:
            greet(index)

    def columns(q):
        return pl.ds(pl.multiple_of(q * C, C), C)

    def load_x():
        return pltpu.make_async_copy(acts_hbm, x_ref, x_sem)

    def load_w(q):
        return pltpu.make_async_copy(w_hbm.at[0, :, columns(q)], w0_ref.at[q], w_sem.at[q])

    def load_g(q):
        return pltpu.make_async_copy(up_hbm.at[:, columns(q)], g_ref.at[q], g_sem.at[q])

    def load_m(q):
        return pltpu.make_async_copy(m_hbm.at[0, :, columns(q)], m0_ref.at[q], m_sem.at[q])

    def load_v(q):
        return pltpu.make_async_copy(v_hbm.at[0, :, columns(q)], v0_ref.at[q], v_sem.at[q])

    load_x().start()
    for q in range(Q):
        load_w(q).start()
        load_g(q).start()
        load_m(q).start()
        load_v(q).start()

    def rows(r):
        return slice(r * RR, (r + 1) * RR)

    def onward(h, q, r):
        return pltpu.make_async_remote_copy(
            src_ref=leaving.at[h, q, :, rows(r)],
            dst_ref=arrived.at[h, q, :, rows(r)],
            send_sem=send_sem.at[h, q, r],
            recv_sem=recv_sem.at[h, q, r],
            device_id={"blk": after},
            device_id_type=MESH,
        )

    def to_relay(h, q, r):
        return pltpu.make_async_remote_copy(
            src_ref=leaving.at[h, q, :, rows(r)],
            dst_ref=relay.at[h, q, r - RB + RELAYED],
            send_sem=send_sem.at[h, q, r],
            recv_sem=relay_recv_sem.at[h, q, r - RB + RELAYED],
            device_id={"blk": via},
            device_id_type=MESH,
        )

    def from_relay(h, q, r):
        return pltpu.make_async_remote_copy(
            src_ref=relay.at[h, q, r - RB + RELAYED],
            dst_ref=arrived.at[h, q, :, rows(r)],
            send_sem=relay_send_sem.at[h, q, r - RB + RELAYED],
            recv_sem=recv_sem.at[h, q, r],
            device_id={"blk": landing},
            device_id_type=MESH,
        )

    def to_helper(h, k, r):
        return pltpu.make_async_remote_copy(
            src_ref=leaving.at[h, h, :, rows(r)],
            dst_ref=back.at[h, k, RB - 1 - r],
            send_sem=send_sem.at[h, h, r],
            recv_sem=back_recv_sem.at[h, k, RB - 1 - r],
            device_id={"blk": helper},
            device_id_type=MESH,
        )

    def from_helper(h, k, r):
        return pltpu.make_async_remote_copy(
            src_ref=back.at[h, k, RB - 1 - r],
            dst_ref=arrived.at[h, h, :, rows(r)],
            send_sem=back_send_sem.at[h, k, RB - 1 - r],
            recv_sem=recv_sem.at[h, h, r],
            device_id={"blk": jnp.where(k == 0, *back_landings)},
            device_id_type=MESH,
        )

    def helped(h, act):
        early = jnp.where(depth == 5, 0, 1) if h == HOPS - 1 else 1
        for k in (early, 1 - early):
            for r in range(RB - BACKWARD_TURN[h], RB):
                if r >= RB - BACKWARD[h]:
                    mine = helps
                else:
                    mine = jnp.logical_and(helps, jnp.logical_and(depth == 3, k == 0))

                @pl.when(mine)
                def _():
                    act(k, r)

    def help_back(h):
        def act(k, r):
            to_helper(h, k, r).wait_recv()
            from_helper(h, k, r).start()

        helped(h, act)

    def turned(h, q, r):
        in_first = RB - BACKWARD[h] - TURNED[0] <= r < RB - BACKWARD_TURN[h]
        in_rest = r >= RB - TURNED[1]
        if in_first and in_rest:
            return q >= 0
        return q == h if in_first else q != h if in_rest else q < 0

    def send(h, q, r):
        if r < RB - RELAYED:
            onward(h, q, r).start()
            return
        if r >= RB - BACKWARD[h]:
            backward = jnp.logical_and(sends_on, q == h)
        elif r >= RB - BACKWARD_TURN[h]:
            backward = jnp.logical_and(turns, q == h)
        else:
            backward = q < 0
        first = jnp.logical_and(turns, turned(h, q, r))

        @pl.when(backward)
        def _():
            to_helper(h, kind, r).start()

        @pl.when(first)
        def _():
            to_relay(h, q, r).start()

        @pl.when(jnp.logical_not(jnp.logical_or(first, backward)))
        def _():
            onward(h, q, r).start()

    def relayed(h, q, act):
        for r in range(RB - RELAYED, RB):

            @pl.when(jnp.logical_and(relays, turned(h, q, r)))
            def _():
                act(r)

    def pass_on(h, q):
        def act(r):
            to_relay(h, q, r).wait_recv()
            from_relay(h, q, r).start()

        relayed(h, q, act)

    def slopes(q, weight):
        preact = jnp.dot(x_ref[...], weight, preferred_element_type=F32)
        s_ref[q] = (g_ref[q].astype(F32) * gelu_slope(preact)).astype(BF16)

    def update(h, q, r, weight, first, second):
        grad = jnp.dot(xt_ref[rows(r), :], s_ref[q], preferred_element_type=F32)
        first = 0.9 * first + 0.1 * grad
        second = 0.95 * second + 0.05 * grad * grad
        leaving[h, q, 0, rows(r)] = (weight.astype(F32) - 0.01 * first / (jnp.sqrt(second) + 1e-08)).astype(BF16)
        leaving[h, q, 1, rows(r)] = first.astype(BF16)
        leaving[h, q, 2, rows(r)] = second.astype(BF16)
        send(h, q, r)

    def cut(h):
        return pltpu.make_async_remote_copy(
            src_ref=given.at[h],
            dst_ref=theirs.at[h],
            send_sem=cut_send_sem.at[h],
            recv_sem=cut_recv_sem.at[h],
            device_id={"shard": 1 - side},
            device_id_type=MESH,
        )

    def cut_part(weights, start, block):
        s_part = jnp.concatenate([s_ref[q, pl.ds(start, HALF), :] for q in range(Q)], axis=1)
        w_part = jnp.concatenate([weights(q)[rows(block), :] for q in range(Q)], axis=1)
        return lax.dot_general(s_part, w_part, (((1,), (1,)), ((), ())), preferred_element_type=F32)

    def cut_grads(h, weights):
        mine = pl.multiple_of(side * HALF, HALF)
        others = pl.multiple_of((1 - side) * HALF, HALF)
        for block in range(RB):
            given[h, :, rows(block)] = cut_part(weights, others, block).astype(BF16)
        cut(h).start()
        for block in range(RB):
            own[h, :, rows(block)] = cut_part(weights, mine, block)

    def cut_done(h):
        cut(h).wait_recv()
        cut_out[h] = (own[h] + theirs[h].astype(F32)).astype(BF16)

    load_x().wait()

    def hop_start(q):
        load_w(q).wait()
        load_g(q).wait()
        slopes(q, w0_ref[q])

    def hop_rest(q):
        load_m(q).wait()
        load_v(q).wait()
        for r in range(RB):
            update(0, q, r, w0_ref[q, rows(r)], m0_ref[q, rows(r)], v0_ref[q, rows(r)])

    hop_start(0)
    for r in range(RB):
        xt_ref[rows(r), :] = x_ref[:, rows(r)].T
    def one(flag):
        return flag.astype(jnp.int32)

    pl.semaphore_wait(barrier, 4 + one(turns) + 2 * one(relays) + one(lands) + 4 * one(helps))
    hop_rest(0)

    @pl.loop(1, Q)
    def _(q):
        hop_start(q)
        hop_rest(q)

    cut_grads(0, lambda q: w0_ref.at[q])

    def turn(h, i):
        return lax.rem(i + h, Q)

    for h in range(1, HOPS):

        @pl.loop(0, 2 if h == 1 else Q)
        def _(i):
            pass_on(h - 1, turn(h - 1, i))

        @pl.loop(0, Q)
        def _(i):
            q = turn(h, i)
            if h == 1:

                @pl.when(i == 1)
                def _():
                    pass_on(h - 1, turn(h - 1, 2))
                    pass_on(h - 1, turn(h - 1, 3))

            else:

                @pl.when(i == Q - 1)
                def _():
                    @pl.loop(0, Q)
                    def _(k):
                        pass_on(h, turn(h, k))

            for r in range(RB):
                onward(h - 1, q, r).wait_recv()
            slopes(q, arrived[h - 1, q, 0])
            for r in range(RB):
                update(
                    h,
                    q,
                    r,
                    arrived[h - 1, q, 0, rows(r)],
                    arrived[h - 1, q, 1, rows(r)].astype(F32),
                    arrived[h - 1, q, 2, rows(r)].astype(F32),
                )

        help_back(h - 1)
        cut_grads(h, lambda q: arrived.at[h - 1, q, 0])
        cut_done(h - 1)

    def settle(q):
        for r in range(RB):
            onward(HOPS - 1, q, r).wait_recv()
            w_out[rows(r), columns(q)] = arrived[HOPS - 1, q, 0, rows(r)]
            m_out[rows(r), columns(q)] = arrived[HOPS - 1, q, 1, rows(r)].astype(F32)
            v_out[rows(r), columns(q)] = arrived[HOPS - 1, q, 2, rows(r)].astype(F32)

    help_back(HOPS - 1)

    @pl.loop(0, 2)
    def _(i):
        settle(turn(HOPS, i))

    cut_done(HOPS - 1)

    @pl.loop(2, Q)
    def _(i):
        settle(turn(HOPS, i))

    for h in range(HOPS):
        cut(h).wait_send()

        @pl.loop(0, Q)
        def _(q):
            for r in range(RB):
                onward(h, q, r).wait_send()

            relayed(h, q, lambda r: from_relay(h, q, r).wait_send())

        helped(h, lambda k, r: from_helper(h, k, r).wait_send())


def deliver(w_in, m_in, v_in, cut_in, w_out, m_out, v_out, cut_out, sem):
    copies = [
        pltpu.make_async_copy(m_in, m_out.at[0], sem.at[0]),
        pltpu.make_async_copy(v_in, v_out.at[0], sem.at[1]),
        pltpu.make_async_copy(cut_in, cut_out, sem.at[2]),
        pltpu.make_async_copy(w_in, w_out.at[0], sem.at[3]),
    ]
    for copy in copies:
        copy.start()
    for copy in copies:
        copy.wait()


def shards(cut_acts, upstream, weights, moment_one, moment_two):
    anywhere = pl.BlockSpec(memory_space=pl.ANY)
    held = pl.BlockSpec(memory_space=pltpu.VMEM)
    trained = pl.pallas_call(
        kernel,
        out_shape=(
            pltpu.VMEM((D, N), BF16),
            pltpu.VMEM((D, N), F32),
            pltpu.VMEM((D, N), F32),
            pltpu.VMEM((HOPS, HALF, D), BF16),
        ),
        in_specs=[anywhere] * 5,
        out_specs=(held,) * 4,
        scratch_shapes=[
            pltpu.VMEM((ROWS, D), BF16),
            pltpu.VMEM((D, ROWS), BF16),
            pltpu.VMEM((Q, ROWS, C), BF16),
            pltpu.VMEM((Q, D, C), BF16),
            pltpu.VMEM((Q, D, C), F32),
            pltpu.VMEM((Q, D, C), F32),
            pltpu.VMEM((HOPS, Q, 3, D, C), BF16),
            pltpu.VMEM((HOPS, Q, 3, D, C), BF16),
            pltpu.VMEM((HOPS, Q, RELAYED, 3, RR, C), BF16),
            pltpu.VMEM((HOPS, 2, MOST_BACK, 3, RR, C), BF16),
            pltpu.VMEM((Q, ROWS, C), BF16),
            pltpu.VMEM((HOPS, HALF, D), F32),
            pltpu.VMEM((HOPS, HALF, D), BF16),
            pltpu.VMEM((HOPS, HALF, D), BF16),
            pltpu.SemaphoreType.DMA,
            pltpu.SemaphoreType.DMA((Q,)),
            pltpu.SemaphoreType.DMA((Q,)),
            pltpu.SemaphoreType.DMA((Q,)),
            pltpu.SemaphoreType.DMA((Q,)),
            pltpu.SemaphoreType.DMA((HOPS, Q, RB)),
            pltpu.SemaphoreType.DMA((HOPS, Q, RB)),
            pltpu.SemaphoreType.DMA((HOPS, Q, RELAYED)),
            pltpu.SemaphoreType.DMA((HOPS, Q, RELAYED)),
            pltpu.SemaphoreType.DMA((HOPS, 2, MOST_BACK)),
            pltpu.SemaphoreType.DMA((HOPS, 2, MOST_BACK)),
            pltpu.SemaphoreType.DMA((HOPS,)),
            pltpu.SemaphoreType.DMA((HOPS,)),
        ],
        compiler_params=pltpu.CompilerParams(
            collective_id=0, has_side_effects=True, vmem_limit_bytes=48 * 2**20
        ),
        name="relay_train",
    )(cut_acts, upstream, weights, moment_one, moment_two)
    return pl.pallas_call(
        deliver,
        out_shape=(
            jax.ShapeDtypeStruct((1, D, N), BF16),
            jax.ShapeDtypeStruct((1, D, N), F32),
            jax.ShapeDtypeStruct((1, D, N), F32),
            jax.ShapeDtypeStruct((HOPS, HALF, D), BF16),
        ),
        in_specs=[held] * 4,
        out_specs=(anywhere,) * 4,
        scratch_shapes=[pltpu.SemaphoreType.DMA((4,))],
        compiler_params=pltpu.CompilerParams(vmem_limit_bytes=2**20),
        name="deliver",
    )(*trained)


def solution(mesh):
    placed = (
        P("blk", None),
        P("blk", "shard"),
        P("blk", None, "shard"),
        P("blk", None, "shard"),
        P("blk", None, "shard"),
    )
    return jax.shard_map(
        shards,
        mesh=mesh,
        in_specs=placed,
        out_specs=(
            P("blk", None, "shard"),
            P("blk", None, "shard"),
            P("blk", None, "shard"),
            P(None, ("blk", "shard"), None),
        ),
        check_vma=False,
    )
```

```python
import functools

import jax
import jax.numpy as jnp
from jax import lax
from jax.experimental import pallas as pl
from jax.experimental.pallas import tpu as pltpu
from jax.sharding import PartitionSpec as P

HOPS = 3
D = 1024
N = 512
ROWS = 512
HALF = ROWS // 2
C = 128
Q = N // C
RB = 4
RR = D // RB
RELAYED = 3
TURNED = (2, 2)
Z = 8
BACKWARD = (2, 2, 0)
BACKWARD_TURN = (2, 2, 3)
MOST_BACK = max(BACKWARD_TURN)
MESH = pl.DeviceIdType.MESH
F32 = jnp.float32
BF16 = jnp.bfloat16


def gelu_slope(values):
    square = values * values
    inner = 0.7978845608 * (values + 0.044715 * square * values)
    tanh_part = jnp.tanh(inner)
    return 0.5 * (1.0 + tanh_part) + 0.5 * values * (1.0 - tanh_part * tanh_part) * 0.7978845608 * (
        1.0 + 0.134145 * square
    )


def kernel(
    acts_hbm,
    up_hbm,
    w_hbm,
    m_hbm,
    v_hbm,
    w_out,
    m_out,
    v_out,
    cut_out,
    x_ref,
    xt_ref,
    g_ref,
    w0_ref,
    m0_ref,
    v0_ref,
    arrived,
    leaving,
    relay,
    back,
    s_ref,
    own,
    theirs,
    given,
    x_sem,
    g_sem,
    w_sem,
    m_sem,
    v_sem,
    send_sem,
    recv_sem,
    relay_send_sem,
    relay_recv_sem,
    back_send_sem,
    back_recv_sem,
    cut_send_sem,
    cut_recv_sem,
):
    n_blk = lax.axis_size("blk")
    me = lax.axis_index("blk")
    side = lax.axis_index("shard")
    after = lax.rem(me + 1, n_blk)
    before = lax.rem(me + n_blk - 1, n_blk)
    on_chip = lax.rem(me, 2)
    depth = lax.rem(me // 2, Z)
    turns = jnp.logical_and(on_chip == 1, depth == Z - 1)
    relays = jnp.logical_and(on_chip == 0, depth == Z - 1)
    lands = jnp.logical_and(on_chip == 0, depth == 0)
    via = lax.rem(me + 2 * Z - 1, n_blk)
    source = lax.rem(me + n_blk - 2 * Z + 1, n_blk)
    landing = lax.rem(me + n_blk - 2 * (Z - 1), n_blk)
    relayer = lax.rem(me + 2 * (Z - 1), n_blk)
    odd = lax.rem(depth, 2) == 1
    sends_on = on_chip == 1
    kind = lax.rem(depth + 1, 2)
    helps = jnp.logical_and(sends_on, odd)

    def chip(here, by):
        return lax.rem(here + n_blk + 2 * by, n_blk)

    helper = jnp.where(
        odd,
        chip(me, jnp.where(depth == 5, -4, 4)),
        chip(me, jnp.where(depth <= 2, 5, -3)),
    )
    back_sources = (
        chip(me, jnp.where(depth == 1, 4, -4)),
        chip(me, jnp.where(depth >= 5, -5, 3)),
    )
    back_landings = (
        chip(me - 1, jnp.where(depth == 1, 5, -3)),
        chip(me - 1, jnp.where(depth >= 5, -4, 4)),
    )
    last_z = lax.rem(depth + Z - 1, Z)
    back_helper = chip(
        me + 1,
        jnp.where(
            lax.rem(last_z, 2) == 1,
            jnp.where(last_z == 5, -5, 3),
            jnp.where(last_z <= 2, 4, -4),
        ),
    )

    barrier = pltpu.get_barrier_semaphore()

    def greet(index):
        pl.semaphore_signal(barrier, inc=1, device_id={"blk": index}, device_id_type=MESH)

    greet(after)
    greet(before)
    pl.semaphore_signal(barrier, inc=1, device_id={"shard": 1 - side}, device_id_type=MESH)

    @pl.when(turns)
    def _():
        greet(via)

    @pl.when(relays)
    def _():
        greet(source)
        greet(landing)

    @pl.when(lands)
    def _():
        greet(relayer)

    @pl.when(sends_on)
    def _():
        greet(helper)

    @pl.when(on_chip == 0)
    def _():
        greet(back_helper)

    @pl.when(helps)
    def _():
        for index in back_sources + back_landings:
            greet(index)

    def columns(q):
        return pl.ds(pl.multiple_of(q * C, C), C)

    def load_x():
        return pltpu.make_async_copy(acts_hbm, x_ref, x_sem)

    def load_w(q):
        return pltpu.make_async_copy(w_hbm.at[0, :, columns(q)], w0_ref.at[q], w_sem.at[q])

    def load_g(q):
        return pltpu.make_async_copy(up_hbm.at[:, columns(q)], g_ref.at[q], g_sem.at[q])

    def load_m(q):
        return pltpu.make_async_copy(m_hbm.at[0, :, columns(q)], m0_ref.at[q], m_sem.at[q])

    def load_v(q):
        return pltpu.make_async_copy(v_hbm.at[0, :, columns(q)], v0_ref.at[q], v_sem.at[q])

    load_x().start()
    for q in range(Q):
        load_w(q).start()
        load_g(q).start()
        load_m(q).start()
        load_v(q).start()

    def rows(r):
        return slice(r * RR, (r + 1) * RR)

    def onward(h, q, r):
        return pltpu.make_async_remote_copy(
            src_ref=leaving.at[h, q, :, rows(r)],
            dst_ref=arrived.at[h, q, :, rows(r)],
            send_sem=send_sem.at[h, q, r],
            recv_sem=recv_sem.at[h, q, r],
            device_id={"blk": after},
            device_id_type=MESH,
        )

    def to_relay(h, q, r):
        return pltpu.make_async_remote_copy(
            src_ref=leaving.at[h, q, :, rows(r)],
            dst_ref=relay.at[h, q, r - RB + RELAYED],
            send_sem=send_sem.at[h, q, r],
            recv_sem=relay_recv_sem.at[h, q, r - RB + RELAYED],
            device_id={"blk": via},
            device_id_type=MESH,
        )

    def from_relay(h, q, r):
        return pltpu.make_async_remote_copy(
            src_ref=relay.at[h, q, r - RB + RELAYED],
            dst_ref=arrived.at[h, q, :, rows(r)],
            send_sem=relay_send_sem.at[h, q, r - RB + RELAYED],
            recv_sem=recv_sem.at[h, q, r],
            device_id={"blk": landing},
            device_id_type=MESH,
        )

    def to_helper(h, k, r):
        return pltpu.make_async_remote_copy(
            src_ref=leaving.at[h, h, :, rows(r)],
            dst_ref=back.at[h, k, RB - 1 - r],
            send_sem=send_sem.at[h, h, r],
            recv_sem=back_recv_sem.at[h, k, RB - 1 - r],
            device_id={"blk": helper},
            device_id_type=MESH,
        )

    def from_helper(h, k, r):
        return pltpu.make_async_remote_copy(
            src_ref=back.at[h, k, RB - 1 - r],
            dst_ref=arrived.at[h, h, :, rows(r)],
            send_sem=back_send_sem.at[h, k, RB - 1 - r],
            recv_sem=recv_sem.at[h, h, r],
            device_id={"blk": jnp.where(k == 0, *back_landings)},
            device_id_type=MESH,
        )

    def helped(h, act):
        early = jnp.where(depth == 5, 0, 1) if h == HOPS - 1 else 1
        for k in (early, 1 - early):
            for r in range(RB - BACKWARD_TURN[h], RB):
                if r >= RB - BACKWARD[h]:
                    mine = helps
                else:
                    mine = jnp.logical_and(helps, jnp.logical_and(depth == 3, k == 0))

                @pl.when(mine)
                def _():
                    act(k, r)

    def help_back(h):
        def act(k, r):
            to_helper(h, k, r).wait_recv()
            from_helper(h, k, r).start()

        helped(h, act)

    def turned(h, q, r):
        in_first = RB - BACKWARD[h] - TURNED[0] <= r < RB - BACKWARD_TURN[h]
        in_rest = r >= RB - TURNED[1]
        if in_first and in_rest:
            return q >= 0
        return q == h if in_first else q != h if in_rest else q < 0

    def send(h, q, r):
        if r < RB - RELAYED:
            onward(h, q, r).start()
            return
        if r >= RB - BACKWARD[h]:
            backward = jnp.logical_and(sends_on, q == h)
        elif r >= RB - BACKWARD_TURN[h]:
            backward = jnp.logical_and(turns, q == h)
        else:
            backward = q < 0
        first = jnp.logical_and(turns, turned(h, q, r))

        @pl.when(backward)
        def _():
            to_helper(h, kind, r).start()

        @pl.when(first)
        def _():
            to_relay(h, q, r).start()

        @pl.when(jnp.logical_not(jnp.logical_or(first, backward)))
        def _():
            onward(h, q, r).start()

    def relayed(h, q, act):
        for r in range(RB - RELAYED, RB):

            @pl.when(jnp.logical_and(relays, turned(h, q, r)))
            def _():
                act(r)

    def pass_on(h, q):
        def act(r):
            to_relay(h, q, r).wait_recv()
            from_relay(h, q, r).start()

        relayed(h, q, act)

    def slopes(q, weight):
        preact = jnp.dot(x_ref[...], weight, preferred_element_type=F32)
        s_ref[q] = (g_ref[q].astype(F32) * gelu_slope(preact)).astype(BF16)

    def update(h, q, r, weight, first, second):
        grad = jnp.dot(xt_ref[rows(r), :], s_ref[q], preferred_element_type=F32)
        first = 0.9 * first + 0.1 * grad
        second = 0.95 * second + 0.05 * grad * grad
        leaving[h, q, 0, rows(r)] = (weight.astype(F32) - 0.01 * first / (jnp.sqrt(second) + 1e-08)).astype(BF16)
        leaving[h, q, 1, rows(r)] = first.astype(BF16)
        leaving[h, q, 2, rows(r)] = second.astype(BF16)
        send(h, q, r)

    def cut(h):
        return pltpu.make_async_remote_copy(
            src_ref=given.at[h],
            dst_ref=theirs.at[h],
            send_sem=cut_send_sem.at[h],
            recv_sem=cut_recv_sem.at[h],
            device_id={"shard": 1 - side},
            device_id_type=MESH,
        )

    def cut_part(weights, start, block):
        s_part = jnp.concatenate([s_ref[q, pl.ds(start, HALF), :] for q in range(Q)], axis=1)
        w_part = jnp.concatenate([weights(q)[rows(block), :] for q in range(Q)], axis=1)
        return lax.dot_general(s_part, w_part, (((1,), (1,)), ((), ())), preferred_element_type=F32)

    def cut_grads(h, weights):
        mine = pl.multiple_of(side * HALF, HALF)
        others = pl.multiple_of((1 - side) * HALF, HALF)
        for block in range(RB):
            given[h, :, rows(block)] = cut_part(weights, others, block).astype(BF16)
        cut(h).start()
        for block in range(RB):
            own[h, :, rows(block)] = cut_part(weights, mine, block)

    def cut_done(h):
        cut(h).wait_recv()
        cut_out[h] = (own[h] + theirs[h].astype(F32)).astype(BF16)

    load_x().wait()

    def hop_start(q):
        load_w(q).wait()
        load_g(q).wait()
        slopes(q, w0_ref[q])

    def hop_rest(q):
        load_m(q).wait()
        load_v(q).wait()
        for r in range(RB):
            update(0, q, r, w0_ref[q, rows(r)], m0_ref[q, rows(r)], v0_ref[q, rows(r)])

    hop_start(0)
    for r in range(RB):
        xt_ref[rows(r), :] = x_ref[:, rows(r)].T
    def one(flag):
        return flag.astype(jnp.int32)

    pl.semaphore_wait(barrier, 4 + one(turns) + 2 * one(relays) + one(lands) + 4 * one(helps))
    hop_rest(0)

    @pl.loop(1, Q)
    def _(q):
        hop_start(q)
        hop_rest(q)

    cut_grads(0, lambda q: w0_ref.at[q])

    def turn(h, i):
        return lax.rem(i + h, Q)

    for h in range(1, HOPS):

        @pl.loop(0, 2 if h == 1 else Q)
        def _(i):
            pass_on(h - 1, turn(h - 1, i))

        @pl.loop(0, Q)
        def _(i):
            q = turn(h, i)
            if h == 1:

                @pl.when(i == 1)
                def _():
                    pass_on(h - 1, turn(h - 1, 2))
                    pass_on(h - 1, turn(h - 1, 3))

            else:

                @pl.when(i == Q - 1)
                def _():
                    @pl.loop(0, Q)
                    def _(k):
                        pass_on(h, turn(h, k))

            for r in range(RB):
                onward(h - 1, q, r).wait_recv()
            slopes(q, arrived[h - 1, q, 0])
            for r in range(RB):
                update(
                    h,
                    q,
                    r,
                    arrived[h - 1, q, 0, rows(r)],
                    arrived[h - 1, q, 1, rows(r)].astype(F32),
                    arrived[h - 1, q, 2, rows(r)].astype(F32),
                )

        help_back(h - 1)
        cut_grads(h, lambda q: arrived.at[h - 1, q, 0])
        cut_done(h - 1)

    def settle(q):
        for r in range(RB):
            onward(HOPS - 1, q, r).wait_recv()
            w_out[rows(r), columns(q)] = arrived[HOPS - 1, q, 0, rows(r)]
            m_out[rows(r), columns(q)] = arrived[HOPS - 1, q, 1, rows(r)].astype(F32)
            v_out[rows(r), columns(q)] = arrived[HOPS - 1, q, 2, rows(r)].astype(F32)

    help_back(HOPS - 1)

    @pl.loop(0, 2)
    def _(i):
        settle(turn(HOPS, i))

    cut_done(HOPS - 1)

    @pl.loop(2, Q)
    def _(i):
        settle(Q - i)

    for h in range(HOPS):
        cut(h).wait_send()

        @pl.loop(0, Q)
        def _(q):
            for r in range(RB):
                onward(h, q, r).wait_send()

            relayed(h, q, lambda r: from_relay(h, q, r).wait_send())

        helped(h, lambda k, r: from_helper(h, k, r).wait_send())


def deliver(w_in, m_in, v_in, cut_in, w_out, m_out, v_out, cut_out, sem):
    copies = [
        pltpu.make_async_copy(m_in, m_out.at[0], sem.at[0]),
        pltpu.make_async_copy(v_in, v_out.at[0], sem.at[1]),
        pltpu.make_async_copy(cut_in, cut_out, sem.at[2]),
        pltpu.make_async_copy(w_in, w_out.at[0], sem.at[3]),
    ]
    for copy in copies:
        copy.start()
    for copy in copies:
        copy.wait()


def shards(cut_acts, upstream, weights, moment_one, moment_two):
    anywhere = pl.BlockSpec(memory_space=pl.ANY)
    held = pl.BlockSpec(memory_space=pltpu.VMEM)
    trained = pl.pallas_call(
        kernel,
        out_shape=(
            pltpu.VMEM((D, N), BF16),
            pltpu.VMEM((D, N), F32),
            pltpu.VMEM((D, N), F32),
            pltpu.VMEM((HOPS, HALF, D), BF16),
        ),
        in_specs=[anywhere] * 5,
        out_specs=(held,) * 4,
        scratch_shapes=[
            pltpu.VMEM((ROWS, D), BF16),
            pltpu.VMEM((D, ROWS), BF16),
            pltpu.VMEM((Q, ROWS, C), BF16),
            pltpu.VMEM((Q, D, C), BF16),
            pltpu.VMEM((Q, D, C), F32),
            pltpu.VMEM((Q, D, C), F32),
            pltpu.VMEM((HOPS, Q, 3, D, C), BF16),
            pltpu.VMEM((HOPS, Q, 3, D, C), BF16),
            pltpu.VMEM((HOPS, Q, RELAYED, 3, RR, C), BF16),
            pltpu.VMEM((HOPS, 2, MOST_BACK, 3, RR, C), BF16),
            pltpu.VMEM((Q, ROWS, C), BF16),
            pltpu.VMEM((HOPS, HALF, D), F32),
            pltpu.VMEM((HOPS, HALF, D), BF16),
            pltpu.VMEM((HOPS, HALF, D), BF16),
            pltpu.SemaphoreType.DMA,
            pltpu.SemaphoreType.DMA((Q,)),
            pltpu.SemaphoreType.DMA((Q,)),
            pltpu.SemaphoreType.DMA((Q,)),
            pltpu.SemaphoreType.DMA((Q,)),
            pltpu.SemaphoreType.DMA((HOPS, Q, RB)),
            pltpu.SemaphoreType.DMA((HOPS, Q, RB)),
            pltpu.SemaphoreType.DMA((HOPS, Q, RELAYED)),
            pltpu.SemaphoreType.DMA((HOPS, Q, RELAYED)),
            pltpu.SemaphoreType.DMA((HOPS, 2, MOST_BACK)),
            pltpu.SemaphoreType.DMA((HOPS, 2, MOST_BACK)),
            pltpu.SemaphoreType.DMA((HOPS,)),
            pltpu.SemaphoreType.DMA((HOPS,)),
        ],
        compiler_params=pltpu.CompilerParams(
            collective_id=0, has_side_effects=True, vmem_limit_bytes=48 * 2**20
        ),
        name="relay_train",
    )(cut_acts, upstream, weights, moment_one, moment_two)
    return pl.pallas_call(
        deliver,
        out_shape=(
            jax.ShapeDtypeStruct((1, D, N), BF16),
            jax.ShapeDtypeStruct((1, D, N), F32),
            jax.ShapeDtypeStruct((1, D, N), F32),
            jax.ShapeDtypeStruct((HOPS, HALF, D), BF16),
        ),
        in_specs=[held] * 4,
        out_specs=(anywhere,) * 4,
        scratch_shapes=[pltpu.SemaphoreType.DMA((4,))],
        compiler_params=pltpu.CompilerParams(vmem_limit_bytes=2**20),
        name="deliver",
    )(*trained)


def solution(mesh):
    placed = (
        P("blk", None),
        P("blk", "shard"),
        P("blk", None, "shard"),
        P("blk", None, "shard"),
        P("blk", None, "shard"),
    )
    return jax.shard_map(
        shards,
        mesh=mesh,
        in_specs=placed,
        out_specs=(
            P("blk", None, "shard"),
            P("blk", None, "shard"),
            P("blk", None, "shard"),
            P(None, ("blk", "shard"), None),
        ),
        check_vma=False,
    )
```
